128 devices in a mesh: dom: 128 (over x, y, z, core).
Axes of the slice: x: 4, y: 4, z: 4, core: 2. Of those that a mesh axis runs over, the one named last changes fastest.
Arguments:
- positions: float32 [3, 524288], P(None, 'dom'), may hold values from -1.5 to 1.5
- velocity: float32 [3, 524288], P(None, 'dom'), may hold values from -6 to 6
- density_weight: float32 [524288], P('dom'), may hold values from 0.5 to 2
- embed_strength: float32 [524288], P('dom'), may hold values from 0.5 to 2
- occupied: int32 [524288], P('dom'), may hold values 0 or 1
- send_list: int32 [128, 8, 8], P('dom'), may hold values from 0 to 31, as said below
- send_count: int32 [128, 8], P('dom'), may hold values from 0 to 8, as said below
- pair_tiles: int32 [4096, 24], P('dom'), may hold values from 0 to 95, as said below
- pair_count: int32 [4096], P('dom'), may hold values from 1 to 24, as said below
- migrate_dest: int32 [4096], P('dom'), may hold values from 0 to 127, as said below
Outputs:
- force: float32 [3, 524288], P(None, 'dom')
- energy: float32 [524288], P('dom')
- moved: float32 [7, 1048576], P(None, 'dom')
- moved_count: int32 [128], P('dom')
The draws below stay inside these ranges and needn't reach their ends.
Inputs may be any that keep to these rules, and one draw needn't show every extreme that they name: `send_list`: for one domain and one offset the entries are distinct local tile indices. send_count[s, k] counts the tiles domain s sends to domain s - o_k; it is 0 where that domain does not exist and 8 for some pairs. `pair_tiles`: entries index the frame of the tile's domain; a tile's entries are distinct and its first entry is its own local index. `pair_count`: the first tile of every domain uses all 24 slots. `migrate_dest`: A tile's new domain is within 4 of its domain; at most 4 tiles go from one domain to any other, at most 64 tiles to one domain, and both bounds are reached in every draw.
All inputs are finite; a program needn't handle non-finite values. No bound on the sum of `occupied` on one device may be relied on, other than what follows from the above.
Results may differ from the reference program's by a relative error of at most 0.0003.
Values sent between devices are 32-bit elements; how exact they have to be, the bound alone decides.
A program may use at most 64 MiB of HBM per device.

```python
import math
import jax
import jax.numpy as jnp
from jax import lax

TILE = 128
TILES_DEV = 32
PAIRS = 24
GMAX = 8
RADIUS = 4
MMAX = 4
SPAN = 8
CAP = 64
DOMAINS = 128
TILES = 4096
ATOMS = 524288


def offset_list_drawn():
    return [position - RADIUS for position in range(RADIUS)] + [position + 1 for position in range(RADIUS)]


def draw_send_list(key, part):
    keys = jax.random.split(key, DOMAINS * SPAN)
    chosen = jax.vmap(lambda single: jax.random.permutation(single, TILES_DEV)[:GMAX])(keys)
    return chosen.reshape(DOMAINS, SPAN, GMAX).astype(jnp.int32)


def draw_send_count(key, part):
    offsets = jnp.array(offset_list_drawn(), dtype=jnp.int32)
    counts = jax.random.randint(jax.random.fold_in(key, 11), (DOMAINS, SPAN), 0, GMAX + 1).astype(jnp.int32)
    source = jnp.arange(DOMAINS, dtype=jnp.int32)[:, None]
    offset_ids = jnp.arange(SPAN, dtype=jnp.int32)[None, :]
    target = source - offsets[None, :]
    counts = jnp.where((source + offset_ids) % SPAN == 0, GMAX, counts)
    counts = jnp.where((target >= 0) & (target < DOMAINS), counts, 0)
    return counts.astype(jnp.int32)


def draw_pair_tiles(key, part):
    frame_size = TILES_DEV + SPAN * GMAX
    scores = jax.random.randint(jax.random.fold_in(key, 21), (TILES, frame_size), 0, 1 << 20).astype(jnp.int32)
    column = jnp.arange(frame_size, dtype=jnp.int32)[None, :]
    scores = scores * frame_size + column
    own_local = (jnp.arange(TILES, dtype=jnp.int32) % TILES_DEV)[:, None]
    scores = jnp.where(column == own_local, (1 << 20) * frame_size + frame_size, scores)
    chosen = jax.lax.top_k(scores, PAIRS)[1]
    return chosen.astype(jnp.int32)


def draw_pair_count(key, part):
    counts = jax.random.randint(jax.random.fold_in(key, 31), (TILES,), 1, PAIRS + 1).astype(jnp.int32)
    first = jnp.arange(TILES, dtype=jnp.int32) % TILES_DEV == 0
    return jnp.where(first, PAIRS, counts).astype(jnp.int32)


def draw_migrate_dest(key, part):
    offsets = jnp.array(offset_list_drawn(), dtype=jnp.int32)
    hottest = jax.random.randint(jax.random.fold_in(key, 41), (), RADIUS, DOMAINS - RADIUS).astype(jnp.int32)
    counts = jax.random.randint(jax.random.fold_in(key, 42), (DOMAINS, SPAN), 0, MMAX + 1).astype(jnp.int32)
    source = jnp.arange(DOMAINS, dtype=jnp.int32)[:, None]
    target = source + offsets[None, :]
    counts = jnp.where((target >= 0) & (target < DOMAINS), counts, 0)
    counts = jnp.where(target == hottest, MMAX, counts)
    counts = jnp.where(source == hottest, 0, counts)
    keys = jax.random.split(jax.random.fold_in(key, 43), DOMAINS)
    orders = jax.vmap(lambda single: jax.random.permutation(single, TILES_DEV))(keys).astype(jnp.int32)
    rank_of = jnp.argsort(orders, axis=1, stable=True).astype(jnp.int32)
    limits = jnp.cumsum(counts, axis=1).astype(jnp.int32)
    which = jnp.sum((rank_of[:, :, None] >= limits[:, None, :]).astype(jnp.int32), axis=2)
    strides = jnp.concatenate([offsets, jnp.zeros((1,), jnp.int32)])
    return (source + strides[which]).reshape(TILES).astype(jnp.int32)


def with_ends(values, stream_key, low, largest):
    index_at = [jax.random.randint(jax.random.fold_in(stream_key, axis), (), 0, length) for axis, length in enumerate(values.shape)]
    longest = values.shape.index(max(values.shape))
    beside = index_at[:longest] + [(index_at[longest] + 1) % values.shape[longest]] + index_at[longest + 1:]
    return values.at[tuple(index_at)].set(low).at[tuple(beside)].set(largest)


def shard_levels(key, shape, shards, smallest, high):
    def one(dim, blocks):
        steps = jax.random.uniform(jax.random.fold_in(jax.random.fold_in(key, 6), dim), (blocks,), jnp.float32, smallest / len(shards), high / len(shards))
        return jnp.repeat(jnp.exp(steps), shape[dim] // blocks).reshape((-1,) + (1,) * (len(shape) - dim - 1))

    factor_of = one(*shards[0])
    for cut in shards[1:]:
        factor_of = factor_of * one(*cut)
    return factor_of


def normal_values(rng, shape, spread, most, cuts=(), kind=jnp.bfloat16):
    loudness = shard_levels(rng, shape, cuts, -0.22, 0.18) if cuts else 1.0
    values = jax.random.normal(rng, shape, jnp.float32) * spread * loudness
    return jnp.minimum(jnp.maximum(values, -most), most).astype(kind)


def setup_inputs(seed: int = 0) -> dict:
    key_list = jax.random.split(jax.random.key(seed), 11)
    return {
        "positions": jnp.clip(jax.random.uniform(key_list[0], (3, ATOMS), jnp.float32, -1.5, 1.5) * shard_levels(key_list[0], (3, ATOMS), ((1, 128),), -0.4, 0.0), -1.5, 1.5),
        "velocity": normal_values(key_list[1], (3, ATOMS), 1.0, 6.0, ((1, 128),), jnp.float32),
        "density_weight": jnp.clip(jnp.exp(math.log(2.0) - 1.3862944 * jax.random.uniform(key_list[2], (ATOMS,), jnp.float32) ** shard_levels(key_list[2], (ATOMS,), ((0, 128),), -0.2, 0.2)), 0.5, 2.0),
        "embed_strength": jnp.clip(jnp.exp(math.log(2.0) - 1.3862944 * jax.random.uniform(key_list[3], (ATOMS,), jnp.float32) ** shard_levels(key_list[3], (ATOMS,), ((0, 128),), -0.2, 0.2)), 0.5, 2.0),
        "occupied": with_ends((jax.random.randint(key_list[4], (ATOMS,), 0, 4) < 3).astype(jnp.int32), jax.random.fold_in(key_list[4], 1), 0, 1),
        "send_list": draw_send_list(jax.random.fold_in(key_list[10], 71), 0),
        "send_count": draw_send_count(jax.random.fold_in(key_list[10], 71), 0),
        "pair_tiles": draw_pair_tiles(jax.random.fold_in(key_list[10], 71), 0),
        "pair_count": draw_pair_count(jax.random.fold_in(key_list[10], 71), 0),
        "migrate_dest": draw_migrate_dest(jax.random.fold_in(key_list[10], 71), 0),
    }


CUTOFF_SQUARE = 4.0
REPULSE = 0.05
TIME_STEP = 0.05
EXACT_PRODUCT = lax.Precision.HIGHEST

def offset_list():
    return [position - RADIUS for position in range(RADIUS)] + [position + 1 for position in range(RADIUS)]

def pair_weights(own_occ, near_occ, slot_list, used_count, tile_ids):
    tile_width = own_occ.shape[-1]
    used_mask = (jnp.arange(slot_list.shape[1], dtype=jnp.int32)[None, :] < used_count[:, None]).astype(jnp.float32)
    itself = (slot_list == tile_ids[:, None]).astype(jnp.float32)
    identity_mask = jnp.eye(tile_width, dtype=jnp.float32)
    weight = used_mask[:, :, None, None] * own_occ[:, None, :, None] * near_occ[:, :, None, :]
    return weight * (1.0 - itself[:, :, None, None] * identity_mask[None, None])

def closeness(own_pos, near_pos):
    distance = jnp.zeros(near_pos.shape[:2] + (own_pos.shape[2], near_pos.shape[3]), jnp.float32)
    for coordinate in range(3):
        difference = own_pos[:, None, coordinate, :, None] - near_pos[:, :, coordinate, None, :]
        distance = distance + difference * difference
    return jnp.maximum(1.0 - distance / CUTOFF_SQUARE, 0.0)

def density_terms(own_pos, own_occ, near_pos, near_chi, near_occ, slot_list, used_count, tile_ids):
    weight = pair_weights(own_occ, near_occ, slot_list, used_count, tile_ids)
    within = closeness(own_pos, near_pos)
    reach_cube = weight * within * within * within
    density = lax.optimization_barrier(jnp.sum(reach_cube * near_chi[:, :, None, :], axis=(1, 3)))
    pair_energy = lax.optimization_barrier(jnp.sum(reach_cube * within, axis=(1, 3)))
    return (density, pair_energy)

def force_terms(own_pos, own_occ, own_chi, own_slope, near_pos, near_chi, near_occ, near_slope, slot_list, used_count, tile_ids):
    weight = pair_weights(own_occ, near_occ, slot_list, used_count, tile_ids)
    within = closeness(own_pos, near_pos)
    square = within * within
    mixed_slope = own_slope[:, None, :, None] * near_chi[:, :, None, :] + near_slope[:, :, None, :] * own_chi[:, None, :, None]
    pair_coef = weight * (2.0 / CUTOFF_SQUARE) * (3.0 * square * mixed_slope + 4.0 * REPULSE * square * within)
    total_coef = lax.optimization_barrier(jnp.sum(pair_coef, axis=(1, 3)))
    pulled = jnp.einsum('bpij,bpcj->bci', pair_coef, near_pos, precision=EXACT_PRODUCT)
    return own_pos * total_coef[:, None, :] - pulled

def ghost_tiles(per_domain, send_list, send_count):
    domains = per_domain.shape[0]
    offsets = jnp.array(offset_list(), dtype=jnp.int32)
    source = jnp.arange(domains, dtype=jnp.int32)[:, None] + offsets[None, :]
    inside = (source >= 0) & (source < domains)
    clipped = jnp.clip(source, 0, domains - 1).astype(jnp.int32)
    offset_ids = jnp.arange(SPAN, dtype=jnp.int32)[None, :]
    tile_list = send_list[clipped, offset_ids]
    counts = send_count[clipped, offset_ids]
    live_mask = inside[:, :, None] & (jnp.arange(GMAX, dtype=jnp.int32)[None, None, :] < counts[:, :, None])
    picked = per_domain[clipped[:, :, None], tile_list]
    live_float = live_mask.astype(jnp.float32).reshape(live_mask.shape + (1,) * (picked.ndim - 3))
    return (picked * live_float).reshape((domains, SPAN * GMAX) + per_domain.shape[2:])

def reference(positions, velocity, density_weight, embed_strength, occupied, send_list, send_count, pair_tiles, pair_count, migrate_dest):
    domains = send_list.shape[0]
    tiles_here = pair_tiles.shape[0] // domains
    tile_width = TILE
    filled = occupied.astype(jnp.float32).reshape(domains, tiles_here, tile_width)
    pos_tiles = positions.reshape(3, domains, tiles_here, tile_width).transpose(1, 2, 0, 3)
    vel_tiles = velocity.reshape(3, domains, tiles_here, tile_width).transpose(1, 2, 0, 3)
    weight_tiles = density_weight.reshape(domains, tiles_here, tile_width)
    embed_tiles = embed_strength.reshape(domains, tiles_here, tile_width)
    packed = jnp.concatenate([pos_tiles, weight_tiles[:, :, None], filled[:, :, None]], axis=2)
    frame_tiles = jnp.concatenate([packed, ghost_tiles(packed, send_list, send_count)], axis=1)
    slot_tiles = pair_tiles.reshape(domains, tiles_here, PAIRS)
    used_tiles = pair_count.reshape(domains, tiles_here)
    tile_ids = jnp.arange(tiles_here, dtype=jnp.int32)

    def density_domain(batch_items):
        native, frames, slot_list, used_count = batch_items
        nearby = frames[slot_list]
        return density_terms(native[:, 0:3], native[:, 4], nearby[:, :, 0:3], nearby[:, :, 3], nearby[:, :, 4], slot_list, used_count, tile_ids)
    density, pair_energy = lax.map(density_domain, (packed, frame_tiles, slot_tiles, used_tiles))
    root_term = jnp.sqrt(1.0 + density)
    slope_tiles = -0.5 * embed_tiles * filled / root_term
    energy_tiles = filled * (-embed_tiles * root_term + 0.5 * REPULSE * pair_energy)
    slope_frame = jnp.concatenate([slope_tiles, ghost_tiles(slope_tiles, send_list, send_count)], axis=1)

    def force_domain(batch_items):
        native, frames, slot_list, used_count, own_slope, frame_slope = batch_items
        nearby = frames[slot_list]
        near_slope = frame_slope[slot_list]
        return force_terms(native[:, 0:3], native[:, 4], native[:, 3], own_slope, nearby[:, :, 0:3], nearby[:, :, 3], nearby[:, :, 4], near_slope, slot_list, used_count, tile_ids)
    force_tiles = lax.map(force_domain, (packed, frame_tiles, slot_tiles, used_tiles, slope_tiles, slope_frame))
    new_vel = vel_tiles + TIME_STEP * force_tiles
    new_pos = pos_tiles + TIME_STEP * new_vel
    payload = jnp.concatenate([new_pos, new_vel, filled[:, :, None]], axis=2).reshape(domains * tiles_here, 7, tile_width)
    onehot = (migrate_dest[:, None] == jnp.arange(domains, dtype=jnp.int32)[None, :]).astype(jnp.int32)
    before = (jnp.cumsum(onehot, axis=0) - onehot).astype(jnp.int32)
    slot_index = lax.optimization_barrier(jnp.sum(onehot * before, axis=1)).astype(jnp.int32)
    moved_tiles = jnp.zeros((domains * CAP, 7, tile_width), jnp.float32).at[migrate_dest * CAP + slot_index].set(payload)
    tile_atoms = lax.optimization_barrier(jnp.sum(occupied.reshape(domains * tiles_here, tile_width), axis=1)).astype(jnp.int32)
    moved_count = lax.optimization_barrier(jnp.sum(onehot * tile_atoms[:, None], axis=0)).astype(jnp.int32)
    force = force_tiles.transpose(2, 0, 1, 3).reshape(3, domains * tiles_here * tile_width)
    energy = energy_tiles.reshape(domains * tiles_here * tile_width)
    moved = moved_tiles.transpose(1, 0, 2).reshape(7, domains * CAP * tile_width)
    return (force, energy, moved, moved_count)
```

```python
import functools

import jax
import jax.numpy as jnp
from jax import lax
from jax.experimental import pallas as pl
from jax.experimental.pallas import tpu as pltpu
from jax.sharding import PartitionSpec as P

MESH = pl.DeviceIdType.MESH
VMEM = pltpu.VMEM
SMEM = pltpu.SMEM
F32 = jnp.float32
BF16 = jnp.bfloat16
I32 = jnp.int32
KEPT = VMEM

OFFSETS = (-4, -3, -2, -1, 1, 2, 3, 4)
WIDE = 128
OWN = 32
GHOST = 64
FRAME = OWN + GHOST
PAIRS = 24
CAP = 64
HAND = 4
FEAT = 32
ROWS = 24
UNITS = 16
LIST = OWN * PAIRS // 2 + PAIRS // 2 + UNITS
STEP = 0.05
EMPTY = 64.0


def round_bf16(value):
    return value.astype(BF16).astype(F32)


def two_parts(value):
    high = round_bf16(value)
    return high, round_bf16(value - high)


def three_parts(value):
    high, middle = two_parts(value)
    return high, middle, round_bf16(value - high - middle)


def peer(shift):
    size = lax.axis_size("dom")
    return (lax.rem(lax.axis_index("dom") + shift + size, size),)


def greet():
    barrier = pltpu.get_barrier_semaphore()
    for shift in OFFSETS:
        pl.semaphore_signal(barrier, inc=1, device_id=peer(shift), device_id_type=MESH)
    return barrier


def send_block(src, dst, send_sem, recv_sem, shift):
    copy = pltpu.make_async_remote_copy(
        src_ref=src,
        dst_ref=dst,
        send_sem=send_sem,
        recv_sem=recv_sem,
        device_id=peer(shift),
        device_id_type=MESH,
    )
    copy.start()
    return copy


def every(start, step):
    return pl.ds(start, 8, stride=step)


def atoms_kernel(
    pos, vel, chi, occ, slist, scount, pack, ghost, send, land, send_sem, recv_sem
):
    barrier = greet()
    flat = pack.reshape(OWN * 8, WIDE)
    for tile in range(OWN):
        columns = pl.ds(tile * WIDE, WIDE)
        flat[pl.ds(tile * 8, 3), :] = pos[:, columns]
        flat[pl.ds(tile * 8 + 3, 3), :] = vel[:, columns]
    for group in range(OWN // 8):
        rows = pl.ds(group * 8, 8)
        flat[every(group * 64 + 6, 8), :] = occ[rows, :].astype(F32)
        flat[every(group * 64 + 7, 8), :] = chi[rows, :]
    slots = lax.broadcasted_iota(I32, (8, WIDE), 0)
    used = scount[...]
    for place in range(8):
        for slot in range(8):
            held = pack[slist[0, place, slot]]
            send[place, pl.ds(slot, 3, stride=8), :] = held[0:3]
            send[place, pl.ds(24 + slot, 1), :] = held[6:7]
            send[place, pl.ds(32 + slot, 1), :] = held[7:8]
        live = jnp.broadcast_to(used[:, place : place + 1], (8, WIDE)) > slots
        filled = send[place, pl.ds(24, 8), :]
        send[place, pl.ds(24, 8), :] = jnp.where(live, filled, 0.0)
    pl.semaphore_wait(barrier, len(OFFSETS))
    copies = [
        send_block(send.at[p], land.at[p], send_sem.at[p], recv_sem.at[p], -shift)
        for p, shift in enumerate(OFFSETS)
    ]
    for copy in copies:
        copy.wait()
    for place in range(8):
        ghost[place] = land[place]


def fields(group, pack, ghost):
    if group < OWN // 8:
        return [pack[every(group * 64 + row, 8), :] for row in (0, 1, 2, 6, 7)]
    return [ghost[group - OWN // 8, pl.ds(row * 8, 8), :] for row in range(5)]


def place_factors(group, pack, ghost):
    x, y, z, filled, chi = fields(group, pack, ghost)
    parts = [two_parts(0.5 * value) for value in (x, y, z)]
    high = [part[0] for part in parts]
    low = [part[1] for part in parts]
    whole = [h + l for h, l in parts]
    norm = whole[0] * whole[0] + whole[1] * whole[1] + whole[2] * whole[2]
    return high, low, whole, norm, filled, chi


def near_rows(high, low, norm, filled):
    one = jnp.ones_like(norm)
    reach_norm = three_parts(-norm - EMPTY * (1.0 - filled))
    return high + low + high + low + list(reach_norm) + [one, one, one]


def own_rows(high, low, norm):
    one = jnp.ones_like(norm)
    twice_high = [2.0 * h for h in high]
    twice_low = [2.0 * l for l in low]
    rows = twice_high + twice_high + twice_low + twice_low
    return rows + [one, one, one] + list(three_parts(1.0 - norm))


def put_rows(ref, group, rows):
    for k, row in enumerate(rows):
        ref[every(group * 8 * len(rows) + k, len(rows)), :] = row


def padded(ref, tile):
    rows = ref[pl.ds(pl.multiple_of(tile * ROWS, 8), ROWS), :]
    return jnp.concatenate([rows, jnp.zeros((FEAT - ROWS, WIDE), F32)], axis=0)


def total_rows(ref):
    return jnp.sum(ref.T, axis=0, keepdims=True)


def density_kernel(
    pack, ghost, embed, pair_tiles, pair_count, dest,
    slope, energy, near, units, trips, slots, counts,
    own_raw, near_raw, own, chis, acc,
):
    pack = pack.reshape(OWN * 8, WIDE)
    zero = jnp.zeros((8, WIDE), F32)
    blank = [zero] * (ROWS - 18)
    for group in range(FRAME // 8):
        high, low, whole, norm, filled, chi = place_factors(group, pack, ghost)
        put_rows(near_raw, group, near_rows(high, low, norm, filled) + blank)
        chis[pl.ds(group * 8, 8), :] = chi
        if group < OWN // 8:
            put_rows(own_raw, group, own_rows(high, low, norm) + blank)
    chis[pl.ds(FRAME, 8), :] = zero
    near[FRAME] = jnp.zeros((FEAT, WIDE), BF16)

    def near_step(tile, carry):
        near[tile] = padded(near_raw, tile).astype(BF16)
        return carry

    lax.fori_loop(0, FRAME, near_step, 0, unroll=8)

    def own_step(tile, carry):
        own[tile] = padded(own_raw, tile).T.astype(BF16)
        for k in range(2):
            acc[k, tile] = jnp.zeros((WIDE, WIDE), F32)
        return carry

    lax.fori_loop(0, OWN, own_step, 0, unroll=4)
    own[OWN] = jnp.zeros((WIDE, FEAT), BF16)

    def list_step(tile, base):
        used = pair_count[tile]
        for k in range(PAIRS // 2):
            first = pair_tiles[2 * k, tile]
            second = jnp.where(2 * k + 1 < used, pair_tiles[2 * k + 1, tile], FRAME)
            units[base + k] = tile * 65536 + first * 256 + second
        return base + (used + 1) // 2

    total = lax.fori_loop(0, OWN, list_step, 0)
    for k in range(UNITS):
        units[total + k] = OWN * 65536 + FRAME * 256 + FRAME
    trips[0] = (total + UNITS - 1) // UNITS

    for k in range(9):
        counts[k] = 0
        for m in range(HAND):
            slots[k * OWN + m] = 0
    me = lax.axis_index("dom")

    def slot_step(tile, carry):
        shift = dest[tile] - me
        k = jnp.where(shift == 0, 8, jnp.where(shift < 0, shift + 4, shift + 3))
        n = counts[k]
        slots[k * OWN + n] = tile
        counts[k] = n + 1
        return carry

    lax.fori_loop(0, OWN, slot_step, 0)

    def trip(step, carry):
        for k in range(UNITS):
            unit = units[step * UNITS + k]
            tile, first, second = unit >> 16, (unit >> 8) & 255, unit & 255
            pair = jnp.concatenate([near[first], near[second]], axis=1)
            s = jnp.dot(own[tile], pair, preferred_element_type=F32)
            r = jnp.maximum(s, 0.0)
            square = r * r
            cube = square * r
            fourth = square * square
            acc[0, tile] += (
                cube[:, :WIDE] * chis[pl.ds(first, 1), :] + cube[:, WIDE:] * chis[pl.ds(second, 1), :]
            )
            acc[1, tile] += fourth[:, :WIDE] + fourth[:, WIDE:]
        return carry

    lax.fori_loop(0, trips[0], trip, 0)

    for tile in range(OWN):
        slope[pl.ds(tile, 1), :] = total_rows(acc[0, tile])
        energy[pl.ds(tile, 1), :] = total_rows(acc[1, tile])
    for group in range(OWN // 8):
        rows = pl.ds(group * 8, 8)
        x, y, z, filled, chi = fields(group, pack, ghost)
        root = jnp.sqrt(1.0 + (slope[rows, :] - filled * chi))
        energy[rows, :] = filled * (0.025 * (energy[rows, :] - filled) - embed[rows, :] * root)
        slope[rows, :] = -0.5 * embed[rows, :] * filled / root


def slopes_kernel(
    slope, slist, counts, ghost_slope, ghost_count,
    send, land, send_count, land_count, send_sem, recv_sem, send_sem2, recv_sem2,
):
    barrier = greet()
    for place in range(8):
        for slot in range(8):
            send[place, pl.ds(slot, 1), :] = slope[pl.ds(slist[0, place, slot], 1), :]
        send_count[place] = jnp.full((8, WIDE), counts[place], I32)
    pl.semaphore_wait(barrier, len(OFFSETS))
    copies = []
    for p, shift in enumerate(OFFSETS):
        copies.append(
            send_block(send.at[p], land.at[p], send_sem.at[p], recv_sem.at[p], -shift)
        )
        copies.append(
            send_block(
                send_count.at[p], land_count.at[7 - p], send_sem2.at[p], recv_sem2.at[7 - p], shift
            )
        )
    for p, copy in enumerate(copies):
        copy.wait_send()
    for p, shift in enumerate(OFFSETS):
        copies[2 * p].wait_recv()
        copies[2 * p + 1].wait_recv()
    for place in range(8):
        ghost_slope[pl.ds(place * 8, 8), :] = land[place]
        ghost_count[pl.ds(place, 1), :] = land_count[place, pl.ds(0, 1), :]


def force_kernel(
    pack, ghost, slope, ghost_slope, near, units, trips, slots, counts, ghost_count,
    force, fresh, source,
    own_raw, near_raw, own, near_more, places, acc,
):
    pack = pack.reshape(OWN * 8, WIDE)
    fresh = fresh.reshape(OWN * 8, WIDE)
    zero = jnp.zeros((8, WIDE), F32)
    one = jnp.ones((8, WIDE), F32)
    for group in range(FRAME // 8):
        high, low, whole, norm, filled, chi = place_factors(group, pack, ghost)
        mine = group < OWN // 8
        slopes = slope[pl.ds(group * 8, 8), :] if mine else ghost_slope[pl.ds(group * 8 - OWN, 8), :]
        chi_high, chi_low = two_parts(15.0 * chi)
        slope_high, slope_low = two_parts(15.0 * slopes)
        extra = [chi_high, chi_low, chi_high, slope_high, slope_low, slope_high]
        put_rows(near_raw, group, [one, one] + extra)
        for axis in range(3):
            places[axis, pl.ds(group * 8, 8), :] = 2.0 * whole[axis]
        if mine:
            chi_high, chi_low = two_parts(chi)
            slope_high, slope_low = two_parts(slopes)
            extra = [slope_high, slope_high, slope_low, chi_high, chi_high, chi_low]
            put_rows(own_raw, group, own_rows(high, low, norm) + extra)
    for axis in range(3):
        places[axis, pl.ds(FRAME, 8), :] = zero
    near_more[FRAME] = jnp.zeros((16, WIDE), BF16)

    def near_step(tile, carry):
        rows = near_raw[pl.ds(pl.multiple_of(tile * 8, 8), 8), :]
        near_more[tile] = jnp.concatenate([rows, zero], axis=0).astype(BF16)
        return carry

    lax.fori_loop(0, FRAME, near_step, 0, unroll=8)

    def own_step(tile, carry):
        own[tile] = padded(own_raw, tile).T.astype(BF16)
        for k in range(4):
            acc[k, tile] = jnp.zeros((WIDE, WIDE), F32)
        return carry

    lax.fori_loop(0, OWN, own_step, 0, unroll=4)
    own[OWN] = jnp.zeros((WIDE, FEAT), BF16)

    end = 0
    for k in range(9):
        k = (0, 1, 2, 3, 8, 4, 5, 6, 7)[k]
        for m in range(OWN if k == 8 else HAND):
            source[end + m] = 8 * HAND + slots[8 * OWN + m] if k == 8 else k * HAND + m
        end += counts[8] if k == 8 else ghost_count[k, 0]

    def rest(slot, carry):
        source[slot] = 8 * HAND + OWN
        return carry

    lax.fori_loop(end, CAP, rest, 0)

    def both(tile):
        more = jnp.concatenate([near[tile, pl.ds(0, 16), :], near_more[tile]], axis=0)
        return jnp.concatenate([near[tile], more], axis=1)

    def trip(step, carry):
        for k in range(UNITS):
            unit = units[step * UNITS + k]
            tile, first, second = unit >> 16, (unit >> 8) & 255, unit & 255
            pair = jnp.concatenate([both(first), both(second)], axis=1)
            s = jnp.dot(own[tile], pair, preferred_element_type=F32)
            r1 = jnp.maximum(s[:, 0:WIDE], 0.0)
            r2 = jnp.maximum(s[:, 2 * WIDE : 3 * WIDE], 0.0)
            c1 = r1 * r1 * s[:, WIDE : 2 * WIDE]
            c2 = r2 * r2 * s[:, 3 * WIDE : 4 * WIDE]
            acc[0, tile] += c1 + c2
            for axis in range(3):
                acc[1 + axis, tile] += (
                    c1 * places[axis, pl.ds(first, 1), :] + c2 * places[axis, pl.ds(second, 1), :]
                )
        return carry

    lax.fori_loop(0, trips[0], trip, 0)

    for tile in range(OWN):
        for k in range(4):
            own_raw[pl.ds(k * OWN + tile, 1), :] = total_rows(acc[k, tile])
    for group in range(OWN // 8):
        filled = pack[every(group * 64 + 6, 8), :]
        for axis in range(3):
            rows = pl.ds(group * 8, 8)
            place = places[axis, rows, :]
            pulled = own_raw[pl.ds((1 + axis) * OWN + group * 8, 8), :]
            push = (place * own_raw[rows, :] - pulled) * (0.1 * filled)
            speed = pack[every(group * 64 + 3 + axis, 8), :] + STEP * push
            fresh[every(group * 64 + axis, 8), :] = pack[every(group * 64 + axis, 8), :] + STEP * speed
            fresh[every(group * 64 + 3 + axis, 8), :] = speed
            near_raw[every(group * 64 + axis, 8), :] = push
        fresh[every(group * 64 + 6, 8), :] = filled
        fresh[every(group * 64 + 7, 8), :] = zero
    for tile in range(OWN):
        force[:, pl.ds(tile * WIDE, WIDE)] = near_raw[pl.ds(tile * 8, 3), :]


def moving_kernel(fresh, slots, pool, send, land, send_sem, recv_sem):
    barrier = greet()
    for place in range(8):
        for m in range(HAND):
            send[place, m] = fresh[slots[place * OWN + m]]
    pl.semaphore_wait(barrier, len(OFFSETS))
    copies = [
        send_block(send.at[p], land.at[7 - p], send_sem.at[p], recv_sem.at[7 - p], shift)
        for p, shift in enumerate(OFFSETS)
    ]
    for tile in range(OWN):
        pool[8 * HAND + tile] = fresh[tile]
    pool[8 * HAND + OWN] = jnp.zeros((8, WIDE), F32)
    for copy in copies:
        copy.wait()
    for place in range(8):
        for m in range(HAND):
            pool[place * HAND + m] = land[place, m]


def placing_kernel(pool, source, moved, count):
    total = jnp.zeros((8, WIDE), F32)
    for slot in range(CAP):
        held = pool[source[slot]]
        total = total + held
        moved[:, pl.ds(slot * WIDE, WIDE)] = held[0:7]
    count[0] = jnp.sum(total[6:7]).astype(I32)


def on(space):
    return pl.BlockSpec(memory_space=space)


def call(kernel, name, ins, outs, scratch, collective=None):
    return pl.pallas_call(
        kernel,
        name=name,
        in_specs=[on(space) for space in ins],
        out_shape=outs,
        out_specs=[on(SMEM if out.dtype == I32 and len(out.shape) == 1 else VMEM) for out in outs],
        scratch_shapes=scratch,
        compiler_params=pltpu.CompilerParams(collective_id=collective, has_side_effects=True),
    )


def plain(*dims, dtype=F32):
    return jax.ShapeDtypeStruct(dims, dtype)


def kept(*dims, dtype=F32):
    return KEPT(dims, dtype)


def near_by(value):
    return pltpu.with_memory_space_constraint(value, VMEM)


def per_device(
    positions,
    velocity,
    density_weight,
    embed_strength,
    occupied,
    send_list,
    send_count,
    pair_tiles,
    pair_count,
    migrate_dest,
):
    dma = pltpu.SemaphoreType.DMA
    chi = density_weight.reshape(OWN, WIDE)
    embed = embed_strength.reshape(OWN, WIDE)
    occ = occupied.reshape(OWN, WIDE)
    pack, ghost = call(
        atoms_kernel,
        "atoms",
        [VMEM] * 4 + [SMEM, VMEM],
        [kept(OWN, 8, WIDE), kept(8, 40, WIDE)],
        [VMEM((8, 40, WIDE), F32), VMEM((8, 40, WIDE), F32), dma((8,)), dma((8,))],
        0,
    )(positions, velocity, chi, occ, send_list, send_count)
    slope, energy, near, units, trips, slots, counts = call(
        density_kernel,
        "density",
        [VMEM] * 3 + [SMEM] * 3,
        [
            kept(OWN, WIDE),
            plain(OWN, WIDE),
            kept(FRAME + 1, FEAT, WIDE, dtype=BF16),
            plain(LIST, dtype=I32),
            plain(1, dtype=I32),
            plain(9 * OWN, dtype=I32),
            plain(9, dtype=I32),
        ],
        [
            VMEM((OWN * ROWS, WIDE), F32),
            VMEM((FRAME * ROWS, WIDE), F32),
            VMEM((OWN + 1, WIDE, FEAT), BF16),
            VMEM((FRAME + 8, WIDE), F32),
            VMEM((2, OWN + 1, WIDE, WIDE), F32),
        ],
    )(near_by(pack), near_by(ghost), embed, pair_tiles.T, pair_count, migrate_dest)
    ghost_slope, ghost_count = call(
        slopes_kernel,
        "slopes",
        [VMEM, SMEM, SMEM],
        [kept(GHOST, WIDE), plain(8, WIDE, dtype=I32)],
        [
            VMEM((8, 8, WIDE), F32),
            VMEM((8, 8, WIDE), F32),
            VMEM((8, 8, WIDE), I32),
            VMEM((8, 8, WIDE), I32),
        ]
        + [dma((8,))] * 4,
        1,
    )(near_by(slope), send_list, counts)
    force, fresh, source = call(
        force_kernel,
        "force",
        [VMEM] * 5 + [SMEM] * 5,
        [plain(3, OWN * WIDE), kept(OWN, 8, WIDE), plain(CAP + OWN + 8, dtype=I32)],
        [
            VMEM((OWN * ROWS, WIDE), F32),
            VMEM((FRAME * 8, WIDE), F32),
            VMEM((OWN + 1, WIDE, FEAT), BF16),
            VMEM((FRAME + 1, 16, WIDE), BF16),
            VMEM((3, FRAME + 8, WIDE), F32),
            VMEM((4, OWN + 1, WIDE, WIDE), F32),
        ],
    )(near_by(pack), near_by(ghost), near_by(slope), near_by(ghost_slope), near_by(near), units, trips, slots, counts, ghost_count)
    (pool,) = call(
        moving_kernel,
        "moving",
        [VMEM, SMEM],
        [kept(8 * HAND + OWN + 1, 8, WIDE)],
        [VMEM((8, HAND, 8, WIDE), F32), VMEM((8, HAND, 8, WIDE), F32), dma((8,)), dma((8,))],
        2,
    )(near_by(fresh), slots)
    moved, moved_count = call(
        placing_kernel,
        "placing",
        [VMEM, SMEM],
        [plain(7, CAP * WIDE), plain(1, dtype=I32)],
        [],
    )(near_by(pool), source)
    return force, energy.reshape(OWN * WIDE), moved, moved_count


def solution(mesh):
    return jax.shard_map(
        per_device,
        mesh=mesh,
        in_specs=(
            P(None, "dom"),
            P(None, "dom"),
            P("dom"),
            P("dom"),
            P("dom"),
            P("dom", None, None),
            P("dom", None),
            P("dom", None),
            P("dom"),
            P("dom"),
        ),
        out_specs=(P(None, "dom"), P("dom"), P(None, "dom"), P("dom")),
        check_vma=False,
    )
```
